32 devices in a mesh: lat: 8 (over y, x, core), lon: 4 (over z).
Axes of the slice: x: 2, y: 2, z: 4, core: 2. Of those that a mesh axis runs over, the one named last changes fastest.
Arguments:
- inputs: bfloat16 [128, 384, 256], P('lat', 'lon'), may hold values from -6 to 6
- first_filter: bfloat16 [3, 3, 256, 256], replicated, may hold values from -0.125 to 0.125
- second_filter: bfloat16 [3, 3, 256, 256], replicated, may hold values from -0.125 to 0.125
- cotangent: bfloat16 [128, 384, 256], P('lat', 'lon'), may hold values from -30 to 30
Outputs:
- input_grad: bfloat16 [128, 384, 256], P('lat', 'lon')
- first_grad: float32 [3, 3, 256, 256], replicated
- second_grad: float32 [3, 3, 256, 256], replicated
The draws below stay inside these ranges and needn't reach their ends.
All inputs are finite; a program needn't handle non-finite values.
Results may differ from the reference program's by a relative error of at most 0.0061.
Values may be sent and summed in bfloat16 or wider, within the bound.
A program may use at most 64 MiB of HBM per device.

```python
import jax
import jax.numpy as jnp
from jax import lax

CH = 256
NLAT = 128
NLON = 384


def draw_cotangent(key, part):
    lat_pos = jnp.arange(NLAT, dtype=jnp.float32)[:, None, None] / NLAT
    lon_pos = jnp.arange(NLON, dtype=jnp.float32)[None, :, None] / NLON
    rough = jax.random.uniform(jax.random.fold_in(key, 7), (NLAT, NLON, 1), jnp.float32, 0.5, 1.5)
    base = jnp.clip(jax.random.normal(key, (NLAT, NLON, CH), jnp.float32), -6.0, 6.0)
    scale = jnp.exp(jnp.log(3.0) * (lat_pos + lon_pos))
    return jnp.clip(base * rough * scale / 3.0, -30.0, 30.0).astype(jnp.bfloat16)


def levels(stream_key, shape, pieces, low, top_value):
    def one(position, shards_of):
        steps = jax.random.uniform(jax.random.fold_in(jax.random.fold_in(stream_key, 6), position), (shards_of,), jnp.float32, low / len(pieces), top_value / len(pieces))
        return jnp.repeat(jnp.exp(steps), shape[position] // shards_of).reshape((-1,) + (1,) * (len(shape) - position - 1))

    level = one(*pieces[0])
    for cut in pieces[1:]:
        level = level * one(*cut)
    return level


def gaussian(stream_key, extent, deviation, reach, cuts=(), kind=jnp.bfloat16):
    result = jax.random.normal(stream_key, extent, jnp.float32) * deviation
    if len(cuts) > 0:
        result = levels(stream_key, extent, cuts, -0.22, 0.18) * result
    return jnp.clip(result, min=-reach, max=reach).astype(kind)


def setup_inputs(seed: int = 0) -> dict:
    keys = jax.random.split(jax.random.key(seed), 5)
    return {
        "inputs": gaussian(keys[0], (NLAT, NLON, CH), 1.0, 6.0, ((0, 8), (1, 4))),
        "first_filter": gaussian(keys[1], (3, 3, CH, CH), (9 * CH) ** -0.5, 0.125),
        "second_filter": gaussian(keys[2], (3, 3, CH, CH), (9 * CH) ** -0.5, 0.125),
        "cotangent": draw_cotangent(jax.random.fold_in(keys[4], 71), 0),
    }


def pad_field(field):
    wrapped = jnp.concatenate([field[:, -1:], field, field[:, :1]], axis=1)
    zeros = jnp.zeros((1,) + wrapped.shape[1:], wrapped.dtype)
    return jnp.concatenate([zeros, wrapped, zeros], axis=0)

def conv_taps(padded, weight, rows, cols, flipped):
    total = jnp.zeros((rows * cols, weight.shape[3] if not flipped else weight.shape[2]), jnp.float32)
    for first in range(3):
        for second in range(3):
            piece = padded[first:first + rows, second:second + cols, :].reshape(rows * cols, -1)
            if flipped:
                total = total + lax.dot_general(piece, weight[2 - first, 2 - second], (((1,), (1,)), ((), ())), preferred_element_type=jnp.float32)
            else:
                total = total + jnp.dot(piece, weight[first, second], preferred_element_type=jnp.float32)
    return total.reshape(rows, cols, -1)

def filter_grad(padded, delta, rows, cols):
    flat = delta.reshape(rows * cols, -1)
    taps = []
    for first in range(3):
        for second in range(3):
            piece = padded[first:first + rows, second:second + cols, :].reshape(rows * cols, -1)
            taps.append(lax.dot_general(piece, flat, (((0,), (0,)), ((), ())), preferred_element_type=jnp.float32))
    return jnp.stack(taps).reshape(3, 3, flat.shape[1], flat.shape[1])

def gelu_value(value):
    return value * 0.5 * (1.0 + jax.scipy.special.erf(value * 0.7071067811865476))

def gelu_slope(value):
    return 0.5 * (1.0 + jax.scipy.special.erf(value * 0.7071067811865476)) + value * jnp.exp(-0.5 * value * value) * 0.3989422804014327

def reference(inputs, first_filter, second_filter, cotangent):
    rows, cols = (inputs.shape[0], inputs.shape[1])
    padded_in = pad_field(inputs)
    hidden_one = conv_taps(padded_in, first_filter, rows, cols, False)
    act = gelu_value(hidden_one).astype(jnp.bfloat16)
    padded_act = pad_field(act)
    hidden_two = conv_taps(padded_act, second_filter, rows, cols, False)
    delta_two = (cotangent.astype(jnp.float32) * gelu_slope(hidden_two)).astype(jnp.bfloat16)
    second_grad = filter_grad(padded_act, delta_two, rows, cols)
    act_grad = conv_taps(pad_field(delta_two), second_filter, rows, cols, True)
    delta_one = (act_grad * gelu_slope(hidden_one)).astype(jnp.bfloat16)
    first_grad = filter_grad(padded_in, delta_one, rows, cols)
    input_grad = conv_taps(pad_field(delta_one), first_filter, rows, cols, True).astype(jnp.bfloat16)
    return (input_grad, first_grad, second_grad)
```

```python
import functools

import jax
import jax.numpy as jnp
from jax import lax
from jax.experimental import pallas as pl
from jax.experimental.pallas import tpu as pltpu
from jax.sharding import PartitionSpec as P

MESH = pl.DeviceIdType.MESH
PARTS = 3


class Plan:
    def __init__(self, mesh, rows):
        self.lat, self.lon = mesh.shape["lat"], mesh.shape["lon"]
        bits = self.lat.bit_length() - 1
        if self.lat != 2**bits or bits < 1:
            raise ValueError("lat size")
        self.groups = [("lat", 2, 2**b) for b in range(1, bits)]
        if self.lon > 1:
            self.groups.append(("lon", self.lon, 1))
        self.rows = rows
        unit = 16 * (self.lat // 2) * self.lon
        self.padded = -(-rows // unit) * unit
        turn = max(1, len(self.groups) // PARTS)
        self.orders = []
        for p in range(PARTS):
            s = (p * turn) % max(1, len(self.groups))
            self.orders.append(self.groups[s:] + self.groups[:s])
        self.peers = sum(size - 1 for _, size, _ in self.groups)
        self.sems = 2 * (1 + self.peers)


def member(group):
    axis, size, stride = group
    return (lax.axis_index(axis) // stride) % size


def peer(group, k):
    axis, size, stride = group
    at = lax.axis_index(axis) + (k - member(group)) * stride
    if axis == "lat":
        return (at, lax.axis_index("lon"))
    return (lax.axis_index("lat"), at)


def partner():
    lat = lax.axis_index("lat")
    return (lat + 1 - 2 * (lat % 2), lax.axis_index("lon"))


class Reduction:
    def __init__(self, plan, index, grad, out, acc, sbuf, rbuf, send_sem, recv_sem):
        self.plan, self.index, self.grad, self.out = plan, index, grad, out
        self.acc, self.sbuf, self.rbuf = acc, sbuf, rbuf
        self.send_sem, self.recv_sem = send_sem, recv_sem
        self.core = lax.axis_index("lat") % 2
        self.sent = []
        self.pending = [[] for _ in range(PARTS)]
        self.used = [0] * PARTS
        self.base = [0] * PARTS
        self.count = [plan.padded] * PARTS
        self.offset = [0] * PARTS
        self.steps = 2 * len(plan.groups) + 2

    def send(self, p, src, dst, device):
        slot = self.used[p]
        self.used[p] += 1
        copy = pltpu.make_async_remote_copy(
            src_ref=src,
            dst_ref=dst,
            send_sem=self.send_sem.at[self.index, p, slot],
            recv_sem=self.recv_sem.at[self.index, p, slot],
            device_id=device,
            device_id_type=MESH,
        )
        copy.start()
        self.sent.append(copy)
        self.pending[p].append(copy)

    def arrive(self, p):
        for copy in self.pending[p]:
            copy.wait_recv()
        self.pending[p] = []

    def halves(self, p):
        rows = self.plan.rows
        block = self.grad[p * rows : (p + 1) * rows, :]
        half = block.shape[1] // 2
        low, high = block[:, :half], block[:, half:]
        first = self.core == 0
        return jnp.where(first, low, high), jnp.where(first, high, low)

    def start(self):
        plan = self.plan
        for p in range(PARTS):
            mine, other = self.halves(p)
            if plan.padded > plan.rows:
                shape = (plan.padded - plan.rows, mine.shape[1])
                tail = pl.ds(plan.rows, plan.padded - plan.rows)
                self.sbuf[self.index, p, tail, :] = jnp.zeros(shape, jnp.bfloat16)
                self.acc[self.index, p, tail, :] = jnp.zeros(shape, jnp.float32)
            self.sbuf[self.index, p, 0 : plan.rows, :] = other.astype(jnp.bfloat16)
            self.acc[self.index, p, 0 : plan.rows, :] = mine
            whole = pl.ds(0, plan.padded)
            self.send(
                p,
                self.sbuf.at[self.index, p, whole],
                self.rbuf.at[self.index, p, whole],
                partner(),
            )

    def step(self, number):
        for p in range(PARTS):
            self.step_part(p, number)

    def step_part(self, p, number):
        order, i = self.plan.orders[p], self.index
        depth = len(order)
        self.arrive(p)
        if number <= depth:
            base, count = self.base[p], self.count[p]
            if number == 0:
                total = self.acc[i, p, 0:count, :]
                total = total + self.rbuf[i, p, 0:count, :].astype(jnp.float32)
                new_base = count
            else:
                group = order[number - 1]
                size = group[1]
                part = count // size
                at = pl.multiple_of(member(group) * part, 16)
                total = self.acc[i, p, pl.ds(pl.multiple_of(base + at, 16), part), :]
                for t in range(size - 1):
                    low = base + t * part
                    total = total + self.rbuf[i, p, low : low + part, :].astype(jnp.float32)
                new_base = base + count
                count = part
                self.offset[p] = self.offset[p] + at
            self.base[p], self.count[p] = new_base, count
            if number < depth:
                self.acc[i, p, new_base : new_base + count, :] = total
                self.sbuf[i, p, new_base : new_base + count, :] = total.astype(jnp.bfloat16)
                group = order[number]
                size = group[1]
                part = count // size
                for t in range(1, size):
                    k = (member(group) + t) % size
                    self.send(
                        p,
                        self.sbuf.at[i, p, pl.ds(pl.multiple_of(new_base + k * part, 16), part)],
                        self.rbuf.at[i, p, pl.ds(new_base + (t - 1) * part, part)],
                        peer(group, k),
                    )
            else:
                at = pl.multiple_of(self.offset[p], 16)
                self.out[self.core, p, pl.ds(at, count), :] = total.astype(jnp.bfloat16)
                self.spread(p, order, depth)
        else:
            self.spread(p, order, 2 * depth - number)

    def spread(self, p, order, level):
        if level > 0:
            group = order[level - 1]
            span = pl.ds(pl.multiple_of(self.offset[p], 16), self.count[p])
            block = self.out.at[self.core, p, span]
            for t in range(1, group[1]):
                k = (member(group) + t) % group[1]
                self.send(p, block, block, peer(group, k))
            self.offset[p] = self.offset[p] - member(group) * self.count[p]
            self.count[p] *= group[1]
        elif level == 0:
            block = self.out.at[self.core, p]
            self.send(p, block, block, partner())

    def finish(self):
        for copy in self.sent:
            copy.wait_send()


def greet(devices):
    barrier = pltpu.get_barrier_semaphore()
    for device in devices:
        pl.semaphore_signal(barrier, inc=1, device_id=device, device_id_type=MESH)
    pl.semaphore_wait(barrier, len(devices))


def reduction_peers(plan):
    found = [partner()]
    for group in plan.groups:
        for t in range(1, group[1]):
            found.append(peer(group, (member(group) + t) % group[1]))
    return found


def sum_kernel(plan, first, second, out_a, out_b, acc, sbuf, rbuf, send_sem, recv_sem):
    greet(reduction_peers(plan))
    scratch = (acc, sbuf, rbuf, send_sem, recv_sem)
    both = [
        Reduction(plan, 0, first, out_a, *scratch),
        Reduction(plan, 1, second, out_b, *scratch),
    ]
    for one in both:
        one.start()
    for number in range(both[0].steps):
        for one in both:
            one.step(number)
    for one in both:
        one.finish()


def reduction_scratch(plan, half):
    return [
        pltpu.VMEM((2, PARTS, 3 * plan.padded, half), jnp.float32),
        pltpu.VMEM((2, PARTS, 3 * plan.padded, half), jnp.bfloat16),
        pltpu.VMEM((2, PARTS, 3 * plan.padded, half), jnp.bfloat16),
        pltpu.SemaphoreType.DMA((2, PARTS, plan.sems)),
        pltpu.SemaphoreType.DMA((2, PARTS, plan.sems)),
    ]


def unpacked(out, plan, shape):
    value = out[:, :, : plan.rows, :].astype(jnp.float32)
    return jnp.concatenate([value[0], value[1]], axis=-1).reshape(shape)


def summed(mesh, first, second):
    shape = first.shape
    rows, half = shape[0] * shape[1] * shape[2] // PARTS, shape[3] // 2
    plan = Plan(mesh, rows)
    out = jax.ShapeDtypeStruct((2, PARTS, plan.padded, half), jnp.bfloat16)
    a, b = pl.pallas_call(
        functools.partial(sum_kernel, plan),
        out_shape=(out, out),
        in_specs=[pl.BlockSpec(memory_space=pltpu.VMEM)] * 2,
        out_specs=[pl.BlockSpec(memory_space=pltpu.VMEM)] * 2,
        scratch_shapes=reduction_scratch(plan, half),
        compiler_params=pltpu.CompilerParams(
            collective_id=0, has_side_effects=True, vmem_limit_bytes=60 * 2**20
        ),
    )(first.reshape(PARTS * rows, 2 * half), second.reshape(PARTS * rows, 2 * half))
    return unpacked(a, plan, shape), unpacked(b, plan, shape)


def extended(block, sides, width):
    for axis, dim in sides:
        count = lax.axis_size(axis)
        forward = [(i, i + 1) for i in range(count - 1)]
        forward.append((count - 1, 0))
        backward = [(target, source) for source, target in forward]
        low = lax.ppermute(
            lax.slice_in_dim(block, block.shape[dim] - width, None, axis=dim), axis, forward
        )
        high = lax.ppermute(lax.slice_in_dim(block, 0, width, axis=dim), axis, backward)
        block = jnp.concatenate([low, block, high], axis=dim)
    return block


def mask_rows(padded, width):
    rows = padded.shape[0] - 2 * width
    position = lax.broadcasted_iota(jnp.int32, (padded.shape[0], 1, 1), 0)
    index = lax.axis_index("lat")
    count = lax.axis_size("lat")
    dropped = (position < width) & (index == 0) | (position >= rows + width) & (index == count - 1)
    return jnp.where(dropped, jnp.zeros((), padded.dtype), padded)


def extend(field):
    padded = extended(field, (("lat", 0), ("lon", 1)), 1)
    return mask_rows(padded, 1)


def conv_taps(padded, weight, rows, cols, flipped):
    total = jnp.zeros(
        (rows * cols, weight.shape[3] if not flipped else weight.shape[2]), jnp.float32
    )
    for first in range(3):
        for second in range(3):
            piece = padded[first : first + rows, second : second + cols, :].reshape(rows * cols, -1)
            if flipped:
                total = total + lax.dot_general(
                    piece,
                    weight[2 - first, 2 - second],
                    (((1,), (1,)), ((), ())),
                    preferred_element_type=jnp.float32,
                )
            else:
                total = total + jnp.dot(
                    piece, weight[first, second], preferred_element_type=jnp.float32
                )
    return total.reshape(rows, cols, -1)


def filter_grad(padded, delta, rows, cols):
    flat = delta.reshape(rows * cols, -1)
    taps = []
    for first in range(3):
        for second in range(3):
            piece = padded[first : first + rows, second : second + cols, :].reshape(rows * cols, -1)
            taps.append(
                lax.dot_general(
                    piece, flat, (((0,), (0,)), ((), ())), preferred_element_type=jnp.float32
                )
            )
    return jnp.stack(taps).reshape(3, 3, flat.shape[1], flat.shape[1])


def gelu_value(value):
    return value * 0.5 * (1.0 + jax.scipy.special.erf(value * 0.7071067811865476))


def gelu_slope(value):
    return (
        0.5 * (1.0 + jax.scipy.special.erf(value * 0.7071067811865476))
        + value * jnp.exp(-0.5 * value * value) * 0.3989422804014327
    )


def body(mesh, inputs, first_filter, second_filter, cotangent):
    rows, cols = (inputs.shape[0], inputs.shape[1])
    padded_in = extend(inputs)
    hidden_one = conv_taps(padded_in, first_filter, rows, cols, False)
    act = gelu_value(hidden_one).astype(jnp.bfloat16)
    padded_act = extend(act)
    hidden_two = conv_taps(padded_act, second_filter, rows, cols, False)
    delta_two = (cotangent.astype(jnp.float32) * gelu_slope(hidden_two)).astype(jnp.bfloat16)
    second_part = filter_grad(padded_act, delta_two, rows, cols)
    act_grad = conv_taps(extend(delta_two), second_filter, rows, cols, True)
    delta_one = (act_grad * gelu_slope(hidden_one)).astype(jnp.bfloat16)
    first_part = filter_grad(padded_in, delta_one, rows, cols)
    first_grad, second_grad = summed(mesh, first_part, second_part)
    input_grad = conv_taps(extend(delta_one), first_filter, rows, cols, True).astype(jnp.bfloat16)
    return (input_grad, first_grad, second_grad)


def solution(mesh):
    in_specs = (P("lat", "lon", None), P(), P(), P("lat", "lon", None))
    out_specs = (P("lat", "lon", None), P(), P())
    return jax.shard_map(functools.partial(body, mesh), mesh=mesh, in_specs=in_specs, out_specs=out_specs, check_vma=False)
```

```python
import functools

import jax
import jax.numpy as jnp
from jax import lax
from jax.experimental import pallas as pl
from jax.experimental.pallas import tpu as pltpu
from jax.sharding import PartitionSpec as P

MESH = pl.DeviceIdType.MESH
PARTS = 3


class Plan:
    def __init__(self, mesh, rows):
        self.lat, self.lon = mesh.shape["lat"], mesh.shape["lon"]
        bits = self.lat.bit_length() - 1
        if self.lat != 2**bits or bits < 1:
            raise ValueError("lat size")
        self.groups = [("lat", 2, 2**b) for b in range(1, bits)]
        if self.lon > 1:
            self.groups.append(("lon", self.lon, 1))
        self.rows = rows
        unit = 16 * (self.lat // 2) * self.lon
        self.padded = -(-rows // unit) * unit
        turn = max(1, len(self.groups) // PARTS)
        self.orders = []
        for p in range(PARTS):
            s = (p * turn) % max(1, len(self.groups))
            self.orders.append(self.groups[s:] + self.groups[:s])
        self.peers = sum(size - 1 for _, size, _ in self.groups)
        self.sems = 2 * (1 + self.peers)


def member(group):
    axis, size, stride = group
    return (lax.axis_index(axis) // stride) % size


def peer(group, k):
    axis, size, stride = group
    at = lax.axis_index(axis) + (k - member(group)) * stride
    if axis == "lat":
        return (at, lax.axis_index("lon"))
    return (lax.axis_index("lat"), at)


def partner():
    lat = lax.axis_index("lat")
    return (lat + 1 - 2 * (lat % 2), lax.axis_index("lon"))


class Reduction:
    def __init__(self, plan, index, grad, out, acc, sbuf, rbuf, send_sem, recv_sem):
        self.plan, self.index, self.grad, self.out = plan, index, grad, out
        self.acc, self.sbuf, self.rbuf = acc, sbuf, rbuf
        self.send_sem, self.recv_sem = send_sem, recv_sem
        self.core = lax.axis_index("lat") % 2
        self.sent = []
        self.pending = [[] for _ in range(PARTS)]
        self.used = [0] * PARTS
        self.base = [0] * PARTS
        self.count = [plan.padded] * PARTS
        self.offset = [0] * PARTS
        self.steps = 2 * len(plan.groups) + 2

    def send(self, p, src, dst, device):
        slot = self.used[p]
        self.used[p] += 1
        copy = pltpu.make_async_remote_copy(
            src_ref=src,
            dst_ref=dst,
            send_sem=self.send_sem.at[self.index, p, slot],
            recv_sem=self.recv_sem.at[self.index, p, slot],
            device_id=device,
            device_id_type=MESH,
        )
        copy.start()
        self.sent.append(copy)
        self.pending[p].append(copy)

    def arrive(self, p):
        for copy in self.pending[p]:
            copy.wait_recv()
        self.pending[p] = []

    def halves(self, p):
        rows = self.plan.rows
        block = self.grad[p * rows : (p + 1) * rows, :]
        half = block.shape[1] // 2
        low, high = block[:, :half], block[:, half:]
        first = self.core == 0
        return jnp.where(first, low, high), jnp.where(first, high, low)

    def start(self):
        for p in range(PARTS):
            self.start_part(p)

    def start_part(self, p):
        plan = self.plan
        mine, other = self.halves(p)
        if plan.padded > plan.rows:
            shape = (plan.padded - plan.rows, mine.shape[1])
            tail = pl.ds(plan.rows, plan.padded - plan.rows)
            self.sbuf[self.index, p, tail, :] = jnp.zeros(shape, jnp.bfloat16)
            self.acc[self.index, p, tail, :] = jnp.zeros(shape, jnp.float32)
        self.sbuf[self.index, p, 0 : plan.rows, :] = other.astype(jnp.bfloat16)
        self.acc[self.index, p, 0 : plan.rows, :] = mine
        whole = pl.ds(0, plan.padded)
        self.send(
            p,
            self.sbuf.at[self.index, p, whole],
            self.rbuf.at[self.index, p, whole],
            partner(),
        )

    def step(self, number):
        for p in range(PARTS):
            self.step_part(p, number)

    def step_part(self, p, number):
        order, i = self.plan.orders[p], self.index
        depth = len(order)
        self.arrive(p)
        if number <= depth:
            base, count = self.base[p], self.count[p]
            if number == 0:
                total = self.acc[i, p, 0:count, :]
                total = total + self.rbuf[i, p, 0:count, :].astype(jnp.float32)
                new_base = count
            else:
                group = order[number - 1]
                size = group[1]
                part = count // size
                at = pl.multiple_of(member(group) * part, 16)
                total = self.acc[i, p, pl.ds(pl.multiple_of(base + at, 16), part), :]
                for t in range(size - 1):
                    low = base + t * part
                    total = total + self.rbuf[i, p, low : low + part, :].astype(jnp.float32)
                new_base = base + count
                count = part
                self.offset[p] = self.offset[p] + at
            self.base[p], self.count[p] = new_base, count
            if number < depth:
                self.acc[i, p, new_base : new_base + count, :] = total
                self.sbuf[i, p, new_base : new_base + count, :] = total.astype(jnp.bfloat16)
                group = order[number]
                size = group[1]
                part = count // size
                for t in range(1, size):
                    k = (member(group) + t) % size
                    self.send(
                        p,
                        self.sbuf.at[i, p, pl.ds(pl.multiple_of(new_base + k * part, 16), part)],
                        self.rbuf.at[i, p, pl.ds(new_base + (t - 1) * part, part)],
                        peer(group, k),
                    )
            else:
                at = pl.multiple_of(self.offset[p], 16)
                self.out[self.core, p, pl.ds(at, count), :] = total.astype(jnp.bfloat16)
                self.spread(p, order, depth)
        else:
            self.spread(p, order, 2 * depth - number)

    def spread(self, p, order, level):
        if level > 0:
            group = order[level - 1]
            span = pl.ds(pl.multiple_of(self.offset[p], 16), self.count[p])
            block = self.out.at[self.core, p, span]
            for t in range(1, group[1]):
                k = (member(group) + t) % group[1]
                self.send(p, block, block, peer(group, k))
            self.offset[p] = self.offset[p] - member(group) * self.count[p]
            self.count[p] *= group[1]
        elif level == 0:
            block = self.out.at[self.core, p]
            self.send(p, block, block, partner())

    def finish(self):
        for copy in self.sent:
            copy.wait_send()


def greet(devices):
    barrier = pltpu.get_barrier_semaphore()
    for device in devices:
        pl.semaphore_signal(barrier, inc=1, device_id=device, device_id_type=MESH)
    pl.semaphore_wait(barrier, len(devices))


def reduction_peers(plan):
    found = [partner()]
    for group in plan.groups:
        for t in range(1, group[1]):
            found.append(peer(group, (member(group) + t) % group[1]))
    return found


def gelu_parts(value):
    half = 0.5 * (1.0 + lax.erf(value * 0.7071067811865476))
    slope = half + value * jnp.exp(-0.5 * value * value) * 0.3989422804014327
    return value * half, slope


class Halo:
    def __init__(self, field, size, wide, edges, lines, got, gathered, corners, send_sem, recv_sem):
        self.field, self.wide, self.edges, self.lines = field, wide, edges, lines
        self.got, self.gathered, self.corners = got, gathered, corners
        self.send_sem, self.recv_sem = send_sem, recv_sem
        self.rows, self.cols, self.ch = size
        self.copies = []

    def put(self, row, values, count):
        cols = self.cols
        at = pl.multiple_of((row + 1) * cols, 16)
        self.wide[self.field, pl.ds(at, count * cols), self.ch : 2 * self.ch] = values.astype(
            jnp.bfloat16
        )
        for k in range(count):
            self.edges[0, pl.ds(row + k, 1), :] = values[k * cols : k * cols + 1, :]
            self.edges[1, pl.ds(row + k, 1), :] = values[(k + 1) * cols - 1 : (k + 1) * cols, :]

    def center(self, start, count):
        return self.wide.at[self.field, pl.ds(start, count), pl.ds(self.ch, self.ch)]

    def send(self):
        f, rows, cols = self.field, self.rows, self.cols
        for side in range(2):
            self.lines[f, side] = self.edges[side].astype(jnp.bfloat16)
        devices = neighbours()
        last = (rows + 1) * cols
        top, bottom = cols, rows * cols
        moves = [
            (self.center(top, cols), self.center(last, cols)),
            (self.center(bottom, cols), self.center(0, cols)),
            (self.lines.at[f, 0], self.got.at[f, 1]),
            (self.lines.at[f, 1], self.got.at[f, 0]),
            (self.center(top, 16), self.corners.at[f, 3]),
            (self.center(top + cols - 16, 16), self.corners.at[f, 2]),
            (self.center(bottom, 16), self.corners.at[f, 1]),
            (self.center(bottom + cols - 16, 16), self.corners.at[f, 0]),
        ]
        for slot, (src, dst) in enumerate(moves):
            copy = pltpu.make_async_remote_copy(
                src_ref=src,
                dst_ref=dst,
                send_sem=self.send_sem.at[f, slot],
                recv_sem=self.recv_sem.at[f, slot],
                device_id=devices[slot],
                device_id_type=MESH,
            )
            copy.start()
            self.copies.append(copy)

    def shift_row(self, p):
        f, cols, ch = self.field, self.cols, self.ch
        at = pl.ds(pl.multiple_of(p * cols, 16), cols)
        row = self.wide[f, at, ch : 2 * ch].astype(jnp.float32)
        self.wide[f, at, 0:ch] = pltpu.roll(row, 1, 0).astype(jnp.bfloat16)
        self.wide[f, at, 2 * ch : 3 * ch] = pltpu.roll(row, cols - 1, 0).astype(jnp.bfloat16)

    def shift(self):
        @pl.loop(1, self.rows + 1)
        def _(p):
            self.shift_row(p)

    def receive(self):
        f, rows, cols, ch = self.field, self.rows, self.cols, self.ch
        for copy in self.copies:
            copy.wait_recv()
        lat, count = lax.axis_index("lat"), lax.axis_size("lat")
        for p, dropped, pair in ((0, lat == 0, 0), (rows + 1, lat == count - 1, 2)):
            keep = jnp.where(dropped, 0.0, 1.0)
            at = pl.ds(p * cols, cols)
            row = self.wide[f, at, ch : 2 * ch].astype(jnp.float32) * keep
            self.wide[f, at, ch : 2 * ch] = row.astype(jnp.bfloat16)
            left = self.corners[f, pair].astype(jnp.float32) * keep
            right = self.corners[f, pair + 1].astype(jnp.float32) * keep
            self.gathered[0, p : p + 1, :] = left[15:16, :]
            self.gathered[1, p : p + 1, :] = right[0:1, :]
            self.shift_row(p)
        for side in range(2):
            self.gathered[side, 1 : rows + 1, :] = self.got[f, side].astype(jnp.float32)
        place = lax.broadcasted_iota(jnp.int32, (16, ch), 0)

        @pl.loop(0, rows + 2)
        def _(p):
            low = pl.ds(pl.multiple_of(p * cols, 16), 16)
            tile = self.wide[f, low, 0:ch].astype(jnp.float32)
            edge = jnp.broadcast_to(self.gathered[0, pl.ds(p, 1), :], (16, ch))
            self.wide[f, low, 0:ch] = jnp.where(place == 0, edge, tile).astype(jnp.bfloat16)
            high = pl.ds(pl.multiple_of(p * cols + cols - 16, 16), 16)
            tile = self.wide[f, high, 2 * ch : 3 * ch].astype(jnp.float32)
            edge = jnp.broadcast_to(self.gathered[1, pl.ds(p, 1), :], (16, ch))
            self.wide[f, high, 2 * ch : 3 * ch] = jnp.where(place == 15, edge, tile).astype(
                jnp.bfloat16
            )

    def conv(self, row, count, weight):
        total = None
        for a in range(3):
            at = pl.ds(pl.multiple_of((row + a) * self.cols, 16), count * self.cols)
            part = jnp.dot(
                self.wide[self.field, at, :], weight[a], preferred_element_type=jnp.float32
            )
            total = part if total is None else total + part
        return total

    def outer(self, delta, grad, a):
        span = self.rows * self.cols
        ch = self.ch
        grad[a * 3 * ch : (a + 1) * 3 * ch, :] = lax.dot_general(
            self.wide[self.field, pl.ds(a * self.cols, span), :],
            delta.wide[delta.field, pl.ds(self.cols, span), ch : 2 * ch],
            (((0,), (0,)), ((), ())),
            preferred_element_type=jnp.float32,
        )

    def finish(self):
        for copy in self.copies:
            copy.wait_send()


def neighbours():
    lat, lon = lax.axis_index("lat"), lax.axis_index("lon")
    lats, lons = lax.axis_size("lat"), lax.axis_size("lon")
    up, down = (lat + lats - 1) % lats, (lat + 1) % lats
    left, right = (lon + lons - 1) % lons, (lon + 1) % lons
    return [
        (up, lon),
        (down, lon),
        (lat, left),
        (lat, right),
        (up, left),
        (up, right),
        (down, left),
        (down, right),
    ]


def main_kernel(plan, size, inputs, filter_one, filter_two, cotangent, *refs):
    input_grad, out_one, out_two = refs[:3]
    wide, edges, lines, got, gathered, corners, halo_send, halo_recv = refs[3:11]
    slope_one, flip_one, flip_two, grad_one, grad_two = refs[11:16]
    scratch = refs[16:]
    rows, cols, ch = size
    step = 4 if rows % 4 == 0 else 1
    greet(neighbours() + reduction_peers(plan))
    x, act, delta_two, delta_one = [
        Halo(f, size, wide, edges, lines, got, gathered, corners, halo_send, halo_recv)
        for f in range(4)
    ]
    sum_one = Reduction(plan, 0, grad_one, out_one, *scratch)
    sum_two = Reduction(plan, 1, grad_two, out_two, *scratch)

    def block(row):
        return pl.ds(pl.multiple_of(row * cols, 16), step * cols)

    @pl.loop(0, rows // step)
    def _(c):
        x.put(c * step, inputs[block(c * step), :].astype(jnp.float32), step)

    x.send()
    x.shift()
    for source, target in ((filter_two, flip_two), (filter_one, flip_one)):

        @pl.loop(0, 3)
        def _(a):
            for b in range(3):
                tap = source[2 - a, (2 - b) * ch : (3 - b) * ch, :]
                target[a, b * ch : (b + 1) * ch, :] = tap.T

    x.receive()

    @pl.loop(0, rows // step)
    def _(c):
        value, slope = gelu_parts(x.conv(c * step, step, filter_one))
        slope_one[block(c * step), :] = slope
        act.put(c * step, value, step)

    act.send()
    act.shift()
    act.receive()

    @pl.loop(0, rows // step)
    def _(c):
        _, slope = gelu_parts(act.conv(c * step, step, filter_two))
        delta_two.put(c * step, cotangent[block(c * step), :].astype(jnp.float32) * slope, step)

    delta_two.send()
    delta_two.shift()
    for a in range(3):
        act.outer(delta_two, grad_two, a)
        sum_two.start_part(a)
    delta_two.receive()
    sum_two.step(0)

    @pl.loop(0, rows // step)
    def _(c):
        back = delta_two.conv(c * step, step, flip_two)
        delta_one.put(c * step, back * slope_one[block(c * step), :], step)

    delta_one.send()
    delta_one.shift()
    sum_two.step(1)
    number = 2
    for a in range(3):
        x.outer(delta_one, grad_one, a)
        sum_one.start_part(a)
        if number < sum_two.steps:
            sum_two.step(number)
            number += 1
    delta_one.receive()
    done = 0
    pieces = 2 if rows // step % 2 == 0 else 1
    for piece in range(pieces):
        sum_one.step(done)
        done += 1
        if number < sum_two.steps:
            sum_two.step(number)
            number += 1
        first = piece * (rows // step // pieces)

        @pl.loop(first, first + rows // step // pieces)
        def _(c):
            out = delta_one.conv(c * step, step, flip_one)
            input_grad[block(c * step), :] = out.astype(jnp.bfloat16)

    while done < sum_one.steps or number < sum_two.steps:
        if done < sum_one.steps:
            sum_one.step(done)
            done += 1
        if number < sum_two.steps:
            sum_two.step(number)
            number += 1
    for one in (x, act, delta_two, delta_one, sum_one, sum_two):
        one.finish()


def reduction_scratch(plan, half):
    return [
        pltpu.VMEM((2, PARTS, 3 * plan.padded, half), jnp.float32),
        pltpu.VMEM((2, PARTS, 3 * plan.padded, half), jnp.bfloat16),
        pltpu.VMEM((2, PARTS, 3 * plan.padded, half), jnp.bfloat16),
        pltpu.SemaphoreType.DMA((2, PARTS, plan.sems)),
        pltpu.SemaphoreType.DMA((2, PARTS, plan.sems)),
    ]


def unpacked(out, plan, shape):
    value = out[:, :, : plan.rows, :].astype(jnp.float32)
    return jnp.concatenate([value[0], value[1]], axis=-1).reshape(shape)


def body(mesh, inputs, first_filter, second_filter, cotangent):
    rows, cols, ch = inputs.shape
    plan = Plan(mesh, 3 * ch)
    if plan.lon < 2 or cols % 16 or rows % 16:
        raise ValueError("block size")
    out = jax.ShapeDtypeStruct((2, PARTS, plan.padded, ch // 2), jnp.bfloat16)
    vmem = pl.BlockSpec(memory_space=pltpu.VMEM)
    flat = (rows * cols, ch)
    input_grad, first, second = pl.pallas_call(
        functools.partial(main_kernel, plan, (rows, cols, ch)),
        out_shape=(jax.ShapeDtypeStruct(flat, jnp.bfloat16), out, out),
        in_specs=[vmem] * 4,
        out_specs=[vmem] * 3,
        scratch_shapes=[
            pltpu.VMEM((4, (rows + 2) * cols, 3 * ch), jnp.bfloat16),
            pltpu.VMEM((2, rows, ch), jnp.float32),
            pltpu.VMEM((4, 2, rows, ch), jnp.bfloat16),
            pltpu.VMEM((4, 2, rows, ch), jnp.bfloat16),
            pltpu.VMEM((2, rows + 8, ch), jnp.float32),
            pltpu.VMEM((4, 4, 16, ch), jnp.bfloat16),
            pltpu.SemaphoreType.DMA((4, 8)),
            pltpu.SemaphoreType.DMA((4, 8)),
            pltpu.VMEM(flat, jnp.float32),
            pltpu.VMEM((3, 3 * ch, ch), jnp.bfloat16),
            pltpu.VMEM((3, 3 * ch, ch), jnp.bfloat16),
            pltpu.VMEM((9 * ch, ch), jnp.float32),
            pltpu.VMEM((9 * ch, ch), jnp.float32),
        ]
        + reduction_scratch(plan, ch // 2),
        compiler_params=pltpu.CompilerParams(
            collective_id=0, has_side_effects=True, vmem_limit_bytes=62 * 2**20
        ),
    )(
        inputs.reshape(flat),
        first_filter.reshape(3, 3 * ch, ch),
        second_filter.reshape(3, 3 * ch, ch),
        cotangent.reshape(flat),
    )
    shape = first_filter.shape
    return (
        input_grad.reshape(inputs.shape),
        unpacked(first, plan, shape),
        unpacked(second, plan, shape),
    )


def solution(mesh):
    in_specs = (P("lat", "lon", None), P(), P(), P("lat", "lon", None))
    out_specs = (P("lat", "lon", None), P(), P())
    return jax.shard_map(functools.partial(body, mesh), mesh=mesh, in_specs=in_specs, out_specs=out_specs, check_vma=False)
```

```python
import functools

import jax
import jax.numpy as jnp
from jax import lax
from jax.experimental import pallas as pl
from jax.experimental.pallas import tpu as pltpu
from jax.sharding import PartitionSpec as P

MESH = pl.DeviceIdType.MESH
PARTS = 3


class Plan:
    def __init__(self, mesh, rows):
        self.lat, self.lon = mesh.shape["lat"], mesh.shape["lon"]
        if self.lat % 2 or self.lat < 4 or self.lon < 2:
            raise ValueError("mesh size")
        across, along = ("lat", self.lat // 2, 2), ("lon", self.lon, 1)
        self.groups = [across, along]
        self.orders = [[across, along], [across, along], [along, across]]
        self.rows = rows
        unit = 16 * (self.lat // 2) * self.lon
        self.padded = -(-rows // unit) * unit
        self.peers = sum(size - 1 for _, size, _ in self.groups)
        self.sems = 2 * (1 + self.peers)


def member(group):
    axis, size, stride = group
    return (lax.axis_index(axis) // stride) % size


def peer(group, k):
    axis, size, stride = group
    at = lax.axis_index(axis) + (k - member(group)) * stride
    if axis == "lat":
        return (at, lax.axis_index("lon"))
    return (lax.axis_index("lat"), at)


def partner():
    lat = lax.axis_index("lat")
    return (lat + 1 - 2 * (lat % 2), lax.axis_index("lon"))


class Reduction:
    def __init__(self, plan, index, grad, out, acc, sbuf, rbuf, send_sem, recv_sem):
        self.plan, self.index, self.grad, self.out = plan, index, grad, out
        self.acc, self.sbuf, self.rbuf = acc, sbuf, rbuf
        self.send_sem, self.recv_sem = send_sem, recv_sem
        self.core = lax.axis_index("lat") % 2
        self.sent = []
        self.pending = [[] for _ in range(PARTS)]
        self.used = [0] * PARTS
        self.base = [0] * PARTS
        self.count = [plan.padded] * PARTS
        self.offset = [0] * PARTS
        self.steps = 2 * len(plan.groups) + 2

    def send(self, p, src, dst, device):
        slot = self.used[p]
        self.used[p] += 1
        copy = pltpu.make_async_remote_copy(
            src_ref=src,
            dst_ref=dst,
            send_sem=self.send_sem.at[self.index, p, slot],
            recv_sem=self.recv_sem.at[self.index, p, slot],
            device_id=device,
            device_id_type=MESH,
        )
        copy.start()
        self.sent.append(copy)
        self.pending[p].append(copy)

    def arrive(self, p):
        for copy in self.pending[p]:
            copy.wait_recv()
        self.pending[p] = []

    def halves(self, p):
        rows = self.plan.rows
        block = self.grad[p * rows : (p + 1) * rows, :]
        half = block.shape[1] // 2
        low, high = block[:, :half], block[:, half:]
        first = self.core == 0
        return jnp.where(first, low, high), jnp.where(first, high, low)

    def start(self):
        for p in range(PARTS):
            self.start_part(p)

    def start_part(self, p):
        plan = self.plan
        mine, other = self.halves(p)
        if plan.padded > plan.rows:
            shape = (plan.padded - plan.rows, mine.shape[1])
            tail = pl.ds(plan.rows, plan.padded - plan.rows)
            self.sbuf[self.index, p, tail, :] = jnp.zeros(shape, jnp.bfloat16)
            self.acc[self.index, p, tail, :] = jnp.zeros(shape, jnp.float32)
        self.sbuf[self.index, p, 0 : plan.rows, :] = other.astype(jnp.bfloat16)
        self.acc[self.index, p, 0 : plan.rows, :] = mine
        whole = pl.ds(0, plan.padded)
        self.send(
            p,
            self.sbuf.at[self.index, p, whole],
            self.rbuf.at[self.index, p, whole],
            partner(),
        )

    def step(self, number):
        for p in range(PARTS):
            self.step_part(p, number)

    def step_part(self, p, number):
        order, i = self.plan.orders[p], self.index
        depth = len(order)
        self.arrive(p)
        if number <= depth:
            base, count = self.base[p], self.count[p]
            if number == 0:
                total = self.acc[i, p, 0:count, :]
                total = total + self.rbuf[i, p, 0:count, :].astype(jnp.float32)
                new_base = count
            else:
                group = order[number - 1]
                size = group[1]
                part = count // size
                at = pl.multiple_of(member(group) * part, 16)
                total = self.acc[i, p, pl.ds(pl.multiple_of(base + at, 16), part), :]
                for t in range(size - 1):
                    low = base + t * part
                    total = total + self.rbuf[i, p, low : low + part, :].astype(jnp.float32)
                new_base = base + count
                count = part
                self.offset[p] = self.offset[p] + at
            self.base[p], self.count[p] = new_base, count
            if number < depth:
                self.acc[i, p, new_base : new_base + count, :] = total
                self.sbuf[i, p, new_base : new_base + count, :] = total.astype(jnp.bfloat16)
                group = order[number]
                size = group[1]
                part = count // size
                for t in range(1, size):
                    k = (member(group) + t) % size
                    self.send(
                        p,
                        self.sbuf.at[i, p, pl.ds(pl.multiple_of(new_base + k * part, 16), part)],
                        self.rbuf.at[i, p, pl.ds(new_base + (t - 1) * part, part)],
                        peer(group, k),
                    )
            else:
                at = pl.multiple_of(self.offset[p], 16)
                self.out[p, pl.ds(at, count), self.lanes()] = total.astype(jnp.bfloat16)
                self.spread(p, order, depth)
        else:
            self.spread(p, order, 2 * depth - number)

    def lanes(self):
        half = self.out.shape[2] // 2
        return pl.ds(pl.multiple_of(self.core * half, half), half)

    def spread(self, p, order, level):
        if level > 0:
            group = order[level - 1]
            span = pl.ds(pl.multiple_of(self.offset[p], 16), self.count[p])
            block = self.out.at[p, span, self.lanes()]
            for t in range(1, group[1]):
                k = (member(group) + t) % group[1]
                self.send(p, block, block, peer(group, k))
            self.offset[p] = self.offset[p] - member(group) * self.count[p]
            self.count[p] *= group[1]
        elif level == 0:
            block = self.out.at[p, pl.ds(0, self.plan.padded), self.lanes()]
            self.send(p, block, block, partner())

    def finish(self):
        for copy in self.sent:
            copy.wait_send()


def greet(devices):
    barrier = pltpu.get_barrier_semaphore()
    for device in devices:
        pl.semaphore_signal(barrier, inc=1, device_id=device, device_id_type=MESH)
    pl.semaphore_wait(barrier, len(devices))


def reduction_peers(plan):
    found = [partner()]
    for group in plan.groups:
        for t in range(1, group[1]):
            found.append(peer(group, (member(group) + t) % group[1]))
    return found


def gelu_parts(value):
    half = 0.5 * (1.0 + lax.erf(value * 0.7071067811865476))
    slope = half + value * jnp.exp(-0.5 * value * value) * 0.3989422804014327
    return value * half, slope


class Halo:
    def __init__(self, field, size, wide, edges, lines, got, gathered, corners, send_sem, recv_sem):
        self.field, self.wide, self.edges, self.lines = field, wide, edges, lines
        self.got, self.gathered, self.corners = got, gathered, corners
        self.send_sem, self.recv_sem = send_sem, recv_sem
        self.rows, self.cols, self.ch = size
        self.copies = []

    def put(self, row, values, count):
        cols = self.cols
        at = pl.multiple_of((row + 1) * cols, 16)
        self.wide[self.field, pl.ds(at, count * cols), self.ch : 2 * self.ch] = values.astype(
            jnp.bfloat16
        )
        for k in range(count):
            self.edges[0, pl.ds(row + k, 1), :] = values[k * cols : k * cols + 1, :]
            self.edges[1, pl.ds(row + k, 1), :] = values[(k + 1) * cols - 1 : (k + 1) * cols, :]

    def center(self, start, count):
        return self.wide.at[self.field, pl.ds(start, count), pl.ds(self.ch, self.ch)]

    def send(self):
        f, rows, cols = self.field, self.rows, self.cols
        for side in range(2):
            self.lines[f, side] = self.edges[side].astype(jnp.bfloat16)
        devices = neighbours()
        last = (rows + 1) * cols
        top, bottom = cols, rows * cols
        moves = [
            (self.center(top, cols), self.center(last, cols)),
            (self.center(bottom, cols), self.center(0, cols)),
            (self.lines.at[f, 0], self.got.at[f, 1]),
            (self.lines.at[f, 1], self.got.at[f, 0]),
            (self.center(top, 16), self.corners.at[f, 3]),
            (self.center(top + cols - 16, 16), self.corners.at[f, 2]),
            (self.center(bottom, 16), self.corners.at[f, 1]),
            (self.center(bottom + cols - 16, 16), self.corners.at[f, 0]),
        ]
        for slot, (src, dst) in enumerate(moves):
            copy = pltpu.make_async_remote_copy(
                src_ref=src,
                dst_ref=dst,
                send_sem=self.send_sem.at[f, slot],
                recv_sem=self.recv_sem.at[f, slot],
                device_id=devices[slot],
                device_id_type=MESH,
            )
            copy.start()
            self.copies.append(copy)

    def shift_row(self, p):
        f, cols, ch = self.field, self.cols, self.ch
        at = pl.ds(pl.multiple_of(p * cols, 16), cols)
        row = self.wide[f, at, ch : 2 * ch].astype(jnp.float32)
        self.wide[f, at, 0:ch] = pltpu.roll(row, 1, 0).astype(jnp.bfloat16)
        self.wide[f, at, 2 * ch : 3 * ch] = pltpu.roll(row, cols - 1, 0).astype(jnp.bfloat16)

    def shift(self):
        @pl.loop(1, self.rows + 1)
        def _(p):
            self.shift_row(p)

    def receive(self):
        f, rows, cols, ch = self.field, self.rows, self.cols, self.ch
        for copy in self.copies:
            copy.wait_recv()
        lat, count = lax.axis_index("lat"), lax.axis_size("lat")
        for p, dropped, pair in ((0, lat == 0, 0), (rows + 1, lat == count - 1, 2)):
            keep = jnp.where(dropped, 0.0, 1.0)
            at = pl.ds(p * cols, cols)
            row = self.wide[f, at, ch : 2 * ch].astype(jnp.float32) * keep
            self.wide[f, at, ch : 2 * ch] = row.astype(jnp.bfloat16)
            left = self.corners[f, pair].astype(jnp.float32) * keep
            right = self.corners[f, pair + 1].astype(jnp.float32) * keep
            self.gathered[0, p : p + 1, :] = left[15:16, :]
            self.gathered[1, p : p + 1, :] = right[0:1, :]
            self.shift_row(p)
        for side in range(2):
            self.gathered[side, 1 : rows + 1, :] = self.got[f, side].astype(jnp.float32)
        place = lax.broadcasted_iota(jnp.int32, (16, ch), 0)

        @pl.loop(0, rows + 2)
        def _(p):
            low = pl.ds(pl.multiple_of(p * cols, 16), 16)
            tile = self.wide[f, low, 0:ch].astype(jnp.float32)
            edge = jnp.broadcast_to(self.gathered[0, pl.ds(p, 1), :], (16, ch))
            self.wide[f, low, 0:ch] = jnp.where(place == 0, edge, tile).astype(jnp.bfloat16)
            high = pl.ds(pl.multiple_of(p * cols + cols - 16, 16), 16)
            tile = self.wide[f, high, 2 * ch : 3 * ch].astype(jnp.float32)
            edge = jnp.broadcast_to(self.gathered[1, pl.ds(p, 1), :], (16, ch))
            self.wide[f, high, 2 * ch : 3 * ch] = jnp.where(place == 15, edge, tile).astype(
                jnp.bfloat16
            )

    def conv(self, row, count, weight):
        pieces = []
        for a in range(3):
            at = pl.ds(pl.multiple_of((row + a) * self.cols, 16), count * self.cols)
            pieces.append(self.wide[self.field, at, :])
        return jnp.dot(
            jnp.concatenate(pieces, axis=1), weight[...], preferred_element_type=jnp.float32
        )

    def outer(self, delta, grad, a):
        span = self.rows * self.cols
        ch = self.ch
        grad[a * 3 * ch : (a + 1) * 3 * ch, :] = lax.dot_general(
            self.wide[self.field, pl.ds(a * self.cols, span), :],
            delta.wide[delta.field, pl.ds(self.cols, span), ch : 2 * ch],
            (((0,), (0,)), ((), ())),
            preferred_element_type=jnp.float32,
        )

    def finish(self):
        for copy in self.copies:
            copy.wait_send()


def neighbours():
    lat, lon = lax.axis_index("lat"), lax.axis_index("lon")
    lats, lons = lax.axis_size("lat"), lax.axis_size("lon")
    up, down = (lat + lats - 1) % lats, (lat + 1) % lats
    left, right = (lon + lons - 1) % lons, (lon + 1) % lons
    return [
        (up, lon),
        (down, lon),
        (lat, left),
        (lat, right),
        (up, left),
        (up, right),
        (down, left),
        (down, right),
    ]


def turn_taps(source, target, ch):
    @pl.loop(0, 9)
    def _(tap):
        origin = pl.multiple_of((8 - tap) * ch, ch)
        at = pl.multiple_of(tap * ch, ch)
        target[pl.ds(at, ch), :] = source[pl.ds(origin, ch), :].T


def main_kernel(plan, size, inputs, filter_one, filter_two, cotangent, *refs):
    input_grad, out_one, out_two = refs[:3]
    wide, edges, lines, got, gathered, corners, halo_send, halo_recv = refs[3:11]
    slope_one, flip_one, flip_two, grad_one, grad_two = refs[11:16]
    scratch = refs[16:]
    rows, cols, ch = size
    step = 8 if rows % 8 == 0 else 1
    greet(neighbours() + reduction_peers(plan))
    x, act, delta_two, delta_one = [
        Halo(f, size, wide, edges, lines, got, gathered, corners, halo_send, halo_recv)
        for f in range(4)
    ]
    sum_one = Reduction(plan, 0, grad_one, out_one, *scratch)
    sum_two = Reduction(plan, 1, grad_two, out_two, *scratch)

    def block(row):
        return pl.ds(pl.multiple_of(row * cols, 16), step * cols)

    @pl.loop(0, rows // step)
    def _(c):
        x.put(c * step, inputs[block(c * step), :].astype(jnp.float32), step)

    x.send()
    x.shift()
    turn_taps(filter_one, flip_one, ch)
    x.receive()

    @pl.loop(0, rows // step)
    def _(c):
        value, slope = gelu_parts(x.conv(c * step, step, filter_one))
        slope_one[block(c * step), :] = slope
        act.put(c * step, value, step)

    act.send()
    act.shift()
    turn_taps(filter_two, flip_two, ch)
    act.receive()

    @pl.loop(0, rows // step)
    def _(c):
        _, slope = gelu_parts(act.conv(c * step, step, filter_two))
        delta_two.put(c * step, cotangent[block(c * step), :].astype(jnp.float32) * slope, step)

    delta_two.send()
    delta_two.shift()
    for a in range(3):
        act.outer(delta_two, grad_two, a)
        sum_two.start_part(a)
    delta_two.receive()
    sum_two.step(0)

    @pl.loop(0, rows // step)
    def _(c):
        back = delta_two.conv(c * step, step, flip_two)
        delta_one.put(c * step, back * slope_one[block(c * step), :], step)

    delta_one.send()
    delta_one.shift()
    for a in range(3):
        x.outer(delta_one, grad_one, a)
        sum_one.start_part(a)
    sum_two.step(1)
    delta_one.receive()
    sum_one.step(0)
    sum_two.step(2)

    @pl.loop(0, rows // step)
    def _(c):
        out = delta_one.conv(c * step, step, flip_one)
        input_grad[block(c * step), :] = out.astype(jnp.bfloat16)

    for number in range(1, sum_one.steps):
        sum_one.step(number)
        if number + 2 < sum_two.steps:
            sum_two.step(number + 2)
    for one in (x, act, delta_two, delta_one, sum_one, sum_two):
        one.finish()


def reduction_scratch(plan, half):
    return [
        pltpu.VMEM((2, PARTS, 3 * plan.padded, half), jnp.float32),
        pltpu.VMEM((2, PARTS, 3 * plan.padded, half), jnp.bfloat16),
        pltpu.VMEM((2, PARTS, 3 * plan.padded, half), jnp.bfloat16),
        pltpu.SemaphoreType.DMA((2, PARTS, plan.sems)),
        pltpu.SemaphoreType.DMA((2, PARTS, plan.sems)),
    ]


def unpacked(out, plan, shape):
    return out[:, : plan.rows, :].astype(jnp.float32).reshape(shape)


def body(mesh, inputs, first_filter, second_filter, cotangent):
    rows, cols, ch = inputs.shape
    plan = Plan(mesh, 3 * ch)
    if cols % 16 or rows % 16:
        raise ValueError("block size")
    out = jax.ShapeDtypeStruct((PARTS, plan.padded, ch), jnp.bfloat16)
    vmem = pl.BlockSpec(memory_space=pltpu.VMEM)
    flat = (rows * cols, ch)
    input_grad, first, second = pl.pallas_call(
        functools.partial(main_kernel, plan, (rows, cols, ch)),
        out_shape=(jax.ShapeDtypeStruct(flat, jnp.bfloat16), out, out),
        in_specs=[vmem] * 4,
        out_specs=[vmem] * 3,
        scratch_shapes=[
            pltpu.VMEM((4, (rows + 2) * cols, 3 * ch), jnp.bfloat16),
            pltpu.VMEM((2, rows, ch), jnp.float32),
            pltpu.VMEM((4, 2, rows, ch), jnp.bfloat16),
            pltpu.VMEM((4, 2, rows, ch), jnp.bfloat16),
            pltpu.VMEM((2, rows + 8, ch), jnp.float32),
            pltpu.VMEM((4, 4, 16, ch), jnp.bfloat16),
            pltpu.SemaphoreType.DMA((4, 8)),
            pltpu.SemaphoreType.DMA((4, 8)),
            pltpu.VMEM(flat, jnp.float32),
            pltpu.VMEM((9 * ch, ch), jnp.bfloat16),
            pltpu.VMEM((9 * ch, ch), jnp.bfloat16),
            pltpu.VMEM((9 * ch, ch), jnp.float32),
            pltpu.VMEM((9 * ch, ch), jnp.float32),
        ]
        + reduction_scratch(plan, ch // 2),
        compiler_params=pltpu.CompilerParams(
            collective_id=0, has_side_effects=True, vmem_limit_bytes=62 * 2**20
        ),
    )(
        inputs.reshape(flat),
        first_filter.reshape(9 * ch, ch),
        second_filter.reshape(9 * ch, ch),
        cotangent.reshape(flat),
    )
    shape = first_filter.shape
    return (
        input_grad.reshape(inputs.shape),
        unpacked(first, plan, shape),
        unpacked(second, plan, shape),
    )


def solution(mesh):
    in_specs = (P("lat", "lon", None), P(), P(), P("lat", "lon", None))
    out_specs = (P("lat", "lon", None), P(), P())
    return jax.shard_map(functools.partial(body, mesh), mesh=mesh, in_specs=in_specs, out_specs=out_specs, check_vma=False)
```
